32 devices in a mesh: group: 8 (over y, x, core), section: 4 (over z).
Axes of the slice: x: 2, y: 2, z: 4, core: 2. Of those that a mesh axis runs over, the one named last changes fastest.
Arguments:
- columns: float32 [8, 8, 16, 8192], P('group', None, None, 'section'), may hold values from -6 to 6
- vectors: bfloat16 [8, 8, 128, 8192], P('group', None, None, 'section'), may hold values from -0.0625 to 0.0625
- factors: float32 [8, 8, 128, 128], P('group'), as said below
- order: int32 [8], P('group'), may hold values from 4096 to 8192
- blocks: int32 [8], P('group'), may hold values from 1 to 8
- live: int32 [8, 8], P('group'), may hold values from 0 to 16
Outputs:
- result: float32 [8, 8, 16, 8192], P('group', None, None, 'section')
The draws below stay inside these ranges and needn't reach their ends.
Inputs may be any that keep to these rules, and one draw needn't show every extreme that they name: `factors`: upper triangular, diagonal entries between one half and two, off-diagonal entries small.
All inputs are finite; a program needn't handle non-finite values.
Results may differ from the reference program's by a relative error of at most 0.0003.
Values sent between devices are 32-bit elements; how exact they have to be, the bound alone decides.
No kernel may reach another device: no remote copies, remote signals or barrier semaphores. Data moves between devices by JAX's collectives and lax.ppermute only.
A program may use at most 64 MiB of HBM per device.

```python
import jax
import jax.numpy as jnp
from jax import lax

N = 8192
BW = 128
NB = 8
SLOTS = 16
GROUPS = 8


def draw_factors(key, part):
    first, second = jax.random.split(jax.random.fold_in(key, 17))
    shape = (GROUPS, NB, BW, BW)
    diag = jax.random.uniform(first, shape[:3], jnp.float32, 0.5, 1.5)
    upper = 0.03 * jax.random.normal(second, shape, jnp.float32)
    strict = jnp.triu(jnp.ones((BW, BW), jnp.float32), 1)
    return upper * strict + diag[..., None] * jnp.eye(BW, dtype=jnp.float32)


def touch_ends(result, key, low, top_value):
    spot = [jax.random.randint(jax.random.fold_in(key, axis), (), 0, length) for axis, length in enumerate(result.shape)]
    longest = result.shape.index(max(result.shape))
    next_to = spot[:longest] + [(spot[longest] + 1) % result.shape[longest]] + spot[longest + 1:]
    return result.at[tuple(spot)].set(low).at[tuple(next_to)].set(top_value)


def level_of(own_key, shape, cuts, low, largest):
    level, own = 1.0, jax.random.fold_in(own_key, 6)
    for dim, shards_of in cuts:
        steps = jnp.exp(jax.random.uniform(jax.random.fold_in(own, dim), (shards_of,), jnp.float32, low / len(cuts), largest / len(cuts)))
        level = level * jnp.repeat(steps, shape[dim] // shards_of).reshape([-1 if axis == dim else 1 for axis in range(len(shape))])
    return level


def centred(rng, dims, spread, limit, pieces=(), kind=jnp.bfloat16):
    loudness = level_of(rng, dims, pieces, -0.22, 0.18) if pieces else 1.0
    values = jax.random.normal(rng, dims, jnp.float32) * spread * loudness
    return jnp.minimum(jnp.maximum(values, -limit), limit).astype(kind)


def setup_inputs(seed: int = 0) -> dict:
    key_list = jax.random.split(jax.random.key(seed), 7)
    return {
        "columns": centred(key_list[0], (GROUPS, GROUPS, SLOTS, N), 1.0, 6.0, ((0, 8), (3, 4)), jnp.float32),
        "vectors": centred(key_list[1], (GROUPS, NB, BW, N), N ** -0.5, 0.0625, ((0, 8), (3, 4))),
        "factors": draw_factors(jax.random.fold_in(key_list[6], 71), 0),
        "order": touch_ends(jax.random.randint(key_list[3], (GROUPS,), N // 2, N + 1), jax.random.fold_in(key_list[3], 1), N // 2, N).astype(jnp.int32),
        "blocks": touch_ends(jax.random.randint(key_list[4], (GROUPS,), 1, NB + 1), jax.random.fold_in(key_list[4], 1), 1, NB).astype(jnp.int32),
        "live": touch_ends(jax.random.randint(key_list[5], (GROUPS, GROUPS), 0, SLOTS + 1), jax.random.fold_in(key_list[5], 1), 0, SLOTS).astype(jnp.int32),
    }


def transform(panel, vectors_g, factors_g, size, count):
    inside = (jnp.arange(N) < size).astype(jnp.float32)
    for index in reversed(range(NB)):
        basis = vectors_g[index].astype(jnp.float32) * inside[None, :]
        active = (index < count).astype(jnp.float32)
        factor = factors_g[index] * active
        inner = jnp.dot(panel, basis.T, precision=lax.Precision.HIGHEST)
        scaled = jnp.dot(inner, factor.T, precision=lax.Precision.HIGHEST)
        panel = panel - jnp.dot(scaled, basis, precision=lax.Precision.HIGHEST)
    return panel


def reference(columns, vectors, factors, order, blocks, live):
    def one_matrix(home):
        panel = columns[:, home].reshape(GROUPS * SLOTS, N)
        panel = transform(panel, vectors[home], factors[home], order[home], blocks[home])
        return panel.reshape(GROUPS, SLOTS, N)

    outcome = lax.map(one_matrix, jnp.arange(GROUPS, dtype=jnp.int32))
    outcome = jnp.transpose(outcome, (1, 0, 2, 3))
    keep = jnp.arange(SLOTS, dtype=jnp.int32)[None, None, :] < live[:, :, None]
    return jnp.where(keep[..., None], outcome, jnp.float32(0.0)).astype(jnp.float32)
```

```python
import jax
import jax.numpy as jnp
from jax import lax
from jax.sharding import PartitionSpec as P

HIGH = lax.Precision.HIGHEST
PER_ROUND = 2


def total(value, axis):
    count = lax.axis_size(axis)
    if count & (count - 1):
        return lax.psum(value, axis)
    step = 1
    while step < count:
        value = value + lax.ppermute(value, axis, [(i, i ^ step) for i in range(count)])
        step *= 2
    return value


def split(value):
    upper = lax.reduce_precision(value, 8, 7)
    return upper.astype(jnp.bfloat16), (value - upper).astype(jnp.bfloat16)


def contract(left, right, dims):
    return lax.dot_general(left, right, (dims, ((), ())), preferred_element_type=jnp.float32)


def shards(columns, vectors, factors, order, blocks, live):
    count, width, rows = vectors.shape[1:]
    slots = columns.shape[2]
    held = lax.all_to_all(columns[0], "group", split_axis=0, concat_axis=0, tiled=True)
    shape = held.shape
    panel = held.reshape(shape[0] * shape[1], rows)

    first_row = lax.axis_index("section") * rows
    inside = first_row + jnp.arange(rows) < order[0]
    basis = jnp.where(inside[None, None, :], vectors[0], jnp.bfloat16(0)).reshape(count * width, rows)
    active = (jnp.arange(count) < blocks[0]).astype(jnp.float32)
    factor = factors[0] * active[:, None, None]

    groups = [range(max(top - PER_ROUND, 0), top) for top in range(count, 0, -PER_ROUND)]
    spans = [slice(g.start * width, g.stop * width) for g in groups]

    pieces, where = [], []
    for g in groups:
        for low in g:
            for high in range(low + 1, g.stop):
                where.append((low, high))
                pieces.append(contract(
                    basis[low * width:(low + 1) * width], basis[high * width:(high + 1) * width], ((1,), (1,))))
    inner_gram = dict(zip(where, total(jnp.stack(pieces), "section")))

    merged = []
    for g in groups:
        table = {}
        for low in reversed(g):
            table[low, low] = factor[low]
            for high in range(low + 1, g.stop):
                acc = sum(
                    jnp.dot(inner_gram[low, mid], table[mid, high], precision=HIGH)
                    for mid in range(low + 1, high + 1))
                table[low, high] = -jnp.dot(factor[low], acc, precision=HIGH)
        zero = jnp.zeros((width, width), jnp.float32)
        merged.append(jnp.concatenate(
            [jnp.concatenate([table.get((a, b), zero) for b in g], axis=1) for a in g], axis=0))

    upper, lower = split(panel)
    both = jnp.concatenate([upper, lower], axis=0)
    twice = contract(both, basis, ((1,), (1,)))
    first = twice[:panel.shape[0]] + twice[panel.shape[0]:]

    done = []
    for index, span in enumerate(spans):
        partial = first[:, span]
        if index:
            cross = contract(basis[span], basis[span.stop:], ((1,), (1,)))
            known = jnp.concatenate(done[::-1], axis=1)
            partial = partial - lax.dot_general(known, cross, (((1,), (1,)), ((), ())), precision=HIGH)
        inner = total(partial, "section")
        done.append(lax.dot_general(inner, merged[index], (((1,), (1,)), ((), ())), precision=HIGH))
    weights = jnp.concatenate(done[::-1], axis=1)
    upper, lower = split(weights)
    update = contract(jnp.concatenate([upper, lower], axis=0), basis, ((1,), (0,)))
    moved = (panel - update[:panel.shape[0]] - update[panel.shape[0]:]).reshape(shape)
    returned = lax.all_to_all(moved, "group", split_axis=0, concat_axis=0, tiled=True)
    keep = jnp.arange(slots)[None, :] < live[0][:, None]
    return jnp.where(keep[:, :, None], returned, jnp.float32(0.0))[None]


def solution(mesh):
    return jax.shard_map(
        shards,
        mesh=mesh,
        in_specs=(
            P("group", None, None, "section"),
            P("group", None, None, "section"),
            P("group", None, None, None),
            P("group"),
            P("group"),
            P("group", None),
        ),
        out_specs=P("group", None, None, "section"),
        check_vma=False,
    )
```

```python
import functools

import jax
import jax.numpy as jnp
from jax import lax
from jax.experimental import pallas as pl
from jax.experimental.pallas import tpu as pltpu
from jax.sharding import PartitionSpec as P


HIGH = lax.Precision.HIGHEST
SMEM = pl.BlockSpec(memory_space=pltpu.SMEM)
VMEM = pl.BlockSpec(memory_space=pltpu.VMEM)
ROWS, INNER = ((1,), (1,)), ((1,), (0,))


def dot(left, right, dims, precision=None):
    return lax.dot_general(
        left, right, (dims, ((), ())), precision=precision, preferred_element_type=jnp.float32)


def split(value):
    upper = lax.reduce_precision(value, 8, 7)
    return jnp.concatenate([upper, value - upper], axis=0).astype(jnp.bfloat16)


def folded(value):
    size = value.shape[0] // 2
    return value[:size] + value[size:]


def exchange(value, axis, step):
    count = lax.axis_size(axis)
    return lax.ppermute(value, axis, [(i, i ^ step) for i in range(count)])


def total(value, axis):
    count = lax.axis_size(axis)
    if count & (count - 1):
        return lax.psum(value, axis)
    step = 1
    while step < count:
        value = value + exchange(value, axis, step)
        step *= 2
    return value


def halving_total(value, axis):
    count = lax.axis_size(axis)
    if count & (count - 1):
        return lax.psum(value, axis)
    me = lax.axis_index(axis)
    steps, step = [], 1
    while step < count:
        half = value.shape[0] // 2
        if value.shape[0] % 2 == 0:
            bit = (me // step) % 2
            keep = lax.dynamic_slice_in_dim(value, bit * half, half, 0)
            give = lax.dynamic_slice_in_dim(value, (1 - bit) * half, half, 0)
            value = keep + exchange(give, axis, step)
            steps.append((step, bit))
        else:
            value = value + exchange(value, axis, step)
        step *= 2
    for step, bit in reversed(steps):
        other = exchange(value, axis, step)
        first = jnp.where(bit == 0, value, other)
        second = jnp.where(bit == 0, other, value)
        value = jnp.concatenate([first, second], axis=0)
    return value


def partner(index, step, count):
    return index ^ step if count & (count - 1) == 0 else (step - index) % count


def reorder(sides, me_ref, held_ref, *outs):
    peers, slots, _ = held_ref.shape
    for number, side in enumerate(sides):
        panel_ref, parts_ref = outs[2 * number:2 * number + 2]
        size = len(side) * slots
        for index, step in enumerate(side):
            block = held_ref[partner(me_ref[0], step, peers)]
            upper = block.astype(jnp.bfloat16)
            panel_ref[index * slots:(index + 1) * slots, :] = block
            parts_ref[index * slots:(index + 1) * slots, :] = upper
            parts_ref[size + index * slots:size + (index + 1) * slots, :] = (
                block - upper.astype(jnp.float32)).astype(jnp.bfloat16)


def turn(blocks_ref, factors_ref, lower_ref, higher_ref):
    pairs = lower_ref.shape[0]
    for index in range(pairs):
        first = 2 * (pairs - 1 - index)
        for ref, block in ((lower_ref, first), (higher_ref, first + 1)):
            ref[index] = jnp.where(block < blocks_ref[0], factors_ref[block], 0.0).T


def place(me_ref, live_ref, *refs):
    *blocks, out = refs
    for step, block in enumerate(blocks):
        home = partner(me_ref[0], step, len(blocks))
        slot = lax.broadcasted_iota(jnp.int32, block.shape, 0)
        out[home] = jnp.where(slot < live_ref[home], block[...], 0.0)


def shards(columns, vectors, factors, order, blocks, live):
    count, width, rows = vectors.shape[1:]
    slots = columns.shape[2]
    peers = lax.axis_size("group")
    me = lax.axis_index("group").astype(jnp.int32)[None]
    quarter = peers // 4
    sides = [
        [*range(quarter), *range(peers - quarter, peers)],
        list(range(quarter, peers - quarter)),
    ]

    held = lax.all_to_all(columns[0], "group", split_axis=0, concat_axis=0, tiled=True)

    first_row = lax.axis_index("section") * rows
    inside = first_row + jnp.arange(rows) < order[0]
    basis = jnp.where(inside[None, :], vectors[0].reshape(count * width, rows), jnp.bfloat16(0))
    basis = lax.optimization_barrier(basis)
    tops = list(range(count, 0, -2))

    def span(low, high):
        return basis[low * width:high * width]

    piece = jax.ShapeDtypeStruct((count // 2, width, width), jnp.float32)
    lower, higher = pl.pallas_call(
        turn, out_shape=[piece, piece], in_specs=[SMEM, VMEM], out_specs=[VMEM] * 2, name="turn",
    )(blocks, factors[0])
    gram = jnp.stack([dot(span(top - 1, top), span(top - 2, top - 1), ROWS) for top in tops])
    gram = halving_total(gram, "section")
    crosses = [dot(span(top - 2, top), span(0, top - 2), ROWS) for top in tops[:-1]]
    batch = (((2,), (1,)), ((0,), (0,)))
    corner = -lax.dot_general(
        lax.dot_general(higher, gram, batch, precision=HIGH), lower, batch, precision=HIGH)
    merged = jnp.concatenate(
        [jnp.concatenate([lower, jnp.zeros_like(lower)], axis=2), jnp.concatenate([corner, higher], axis=2)],
        axis=1)

    outs = []
    for side in sides:
        size = len(side) * slots
        outs.append(jax.ShapeDtypeStruct((size, rows), jnp.float32))
        outs.append(jax.ShapeDtypeStruct((2 * size, rows), jnp.bfloat16))
    ordered = pl.pallas_call(
        functools.partial(reorder, sides),
        out_shape=outs, in_specs=[SMEM, VMEM], out_specs=[VMEM] * len(outs), name="reorder",
    )(me, held)

    returned = {}
    for number, side in enumerate(sides):
        panel, parts = ordered[2 * number:2 * number + 2]
        waiting = folded(dot(parts, basis, ROWS))
        known = []
        for index, top in enumerate(tops):
            inner = total(waiting[:, (top - 2) * width:], "section")
            weights = dot(inner, merged[index], INNER, HIGH)
            known.insert(0, weights)
            if top > 2:
                waiting = waiting[:, :(top - 2) * width] - dot(weights, crosses[index], INNER, HIGH)
        moved = panel - folded(dot(split(jnp.concatenate(known, axis=1)), basis, INNER))
        for index, step in enumerate(side):
            block = moved[index * slots:(index + 1) * slots]
            if step or peers & (peers - 1):
                pairs = [(i, partner(i, step, peers)) for i in range(peers)]
                block = lax.ppermute(block, "group", pairs)
            returned[step] = block

    return pl.pallas_call(
        place,
        out_shape=jax.ShapeDtypeStruct(columns.shape[1:], jnp.float32),
        in_specs=[SMEM, SMEM] + [VMEM] * peers, out_specs=VMEM, name="place",
    )(me, live[0], *[returned[step] for step in range(peers)])[None]


def solution(mesh):
    return jax.shard_map(
        shards,
        mesh=mesh,
        in_specs=(
            P("group", None, None, "section"),
            P("group", None, None, "section"),
            P("group", None, None, None),
            P("group"),
            P("group"),
            P("group", None),
        ),
        out_specs=P("group", None, None, "section"),
        check_vma=False,
    )
```

```python
import jax
import jax.numpy as jnp
from jax import lax
from jax.experimental import pallas as pl
from jax.experimental.pallas import tpu as pltpu
from jax.sharding import PartitionSpec as P


HIGH = lax.Precision.HIGHEST
SMEM = pl.BlockSpec(memory_space=pltpu.SMEM)
VMEM = pl.BlockSpec(memory_space=pltpu.VMEM)
ROWS, INNER = ((1,), (1,)), ((1,), (0,))


def dot(left, right, dims, precision=None):
    return lax.dot_general(
        left, right, (dims, ((), ())), precision=precision, preferred_element_type=jnp.float32)


def split(value):
    upper = lax.reduce_precision(value, 8, 7)
    return jnp.concatenate([upper, value - upper], axis=0).astype(jnp.bfloat16)


def folded(value):
    size = value.shape[0] // 2
    return value[:size] + value[size:]


def exchange(value, axis, step):
    count = lax.axis_size(axis)
    return lax.ppermute(value, axis, [(i, i ^ step) for i in range(count)])


def total(value, axis):
    count = lax.axis_size(axis)
    if count & (count - 1):
        return lax.psum(value, axis)
    step = 1
    while step < count:
        value = value + exchange(value, axis, step)
        step *= 2
    return value


def turn(blocks_ref, factors_ref, *outs):
    pairs = factors_ref.shape[0] // 2
    for index in range(pairs):
        first = 2 * (pairs - 1 - index)
        for ref, block in zip(outs[2 * min(index, 1):], (first, first + 1)):
            ref[max(index - 1, 0)] = jnp.where(block < blocks_ref[0], factors_ref[block], 0.0).T


def shards(columns, vectors, factors, order, blocks, live):
    count, width, rows = vectors.shape[1:]
    slots = columns.shape[2]
    pairs = count // 2
    turns = list(reversed(range(pairs)))

    held = lax.all_to_all(columns[0], "group", split_axis=0, concat_axis=0, tiled=True)

    inside = lax.axis_index("section") * rows + jnp.arange(rows) < order[0]
    basis = jnp.where(inside[None, :], vectors[0].reshape(count * width, rows), jnp.bfloat16(0))
    basis = lax.optimization_barrier(basis)

    def span(low, high):
        return basis[low * width:high * width]

    def product(pair):
        return dot(span(2 * pair + 1, 2 * pair + 2), span(2 * pair, 2 * pair + 1), ROWS)

    gram_first = total(product(turns[0])[None], "section")
    rest = jnp.stack([product(pair) for pair in turns[1:]])
    gram_rest = total(rest, "section")
    outs = [jax.ShapeDtypeStruct((size, width, width), jnp.float32) for size in (1, 1, pairs - 1, pairs - 1)]
    turned = pl.pallas_call(
        turn, out_shape=outs, in_specs=[SMEM, VMEM], out_specs=[VMEM] * 4, name="turn",
    )(blocks, factors[0])

    def merge(gram, lower, higher):
        batch = (((2,), (1,)), ((0,), (0,)))
        corner = -lax.dot_general(
            lax.dot_general(higher, gram, batch, precision=HIGH), lower, batch, precision=HIGH)
        return jnp.concatenate([
            jnp.concatenate([lower, jnp.zeros_like(lower)], axis=2),
            jnp.concatenate([corner, higher], axis=2)], axis=1)

    merged = [merge(gram_first, *turned[:2])[0]]
    rest = merge(gram_rest, *turned[2:])
    merged += [rest[index] for index in range(pairs - 1)]

    half = held.shape[0] // 2
    panels = [held[number * half:(number + 1) * half].reshape(half * slots, rows) for number in range(2)]
    for index, pair in enumerate(turns):
        vectors_of = span(2 * pair, 2 * pair + 2)
        for number, panel in enumerate(panels):
            inner = folded(dot(split(panel), vectors_of, ROWS))
            inner = total(inner, "section")
            weights = dot(inner, merged[index], INNER, HIGH)
            panels[number] = panel - folded(dot(split(weights), vectors_of, INNER))
    moved = [panel.reshape(half, slots, rows) for panel in panels]

    returned = lax.all_to_all(
        jnp.concatenate(moved, axis=0), "group", split_axis=0, concat_axis=0, tiled=True)
    keep = jnp.arange(slots)[None, :] < live[0][:, None]
    return jnp.where(keep[:, :, None], returned, jnp.float32(0.0))[None]


def solution(mesh):
    return jax.shard_map(
        shards,
        mesh=mesh,
        in_specs=(
            P("group", None, None, "section"),
            P("group", None, None, "section"),
            P("group", None, None, None),
            P("group"),
            P("group"),
            P("group", None),
        ),
        out_specs=P("group", None, None, "section"),
        check_vma=False,
    )
```

```python
import jax
import jax.numpy as jnp
from jax import lax
from jax.experimental import pallas as pl
from jax.experimental.pallas import tpu as pltpu
from jax.sharding import PartitionSpec as P


HIGH = lax.Precision.HIGHEST
SMEM = pl.BlockSpec(memory_space=pltpu.SMEM)
VMEM = pl.BlockSpec(memory_space=pltpu.VMEM)
ROWS, INNER = ((1,), (1,)), ((1,), (0,))


def dot(left, right, dims, precision=None):
    return lax.dot_general(
        left, right, (dims, ((), ())), precision=precision, preferred_element_type=jnp.float32)


def split(value):
    upper = lax.reduce_precision(value, 8, 7)
    return jnp.concatenate([upper, value - upper], axis=0).astype(jnp.bfloat16)


def folded(value):
    size = value.shape[0] // 2
    return value[:size] + value[size:]


def exchange(value, axis, step):
    count = lax.axis_size(axis)
    return lax.ppermute(value, axis, [(i, i ^ step) for i in range(count)])


def total(value, axis):
    count = lax.axis_size(axis)
    if count & (count - 1):
        return lax.psum(value, axis)
    step = 1
    while step < count:
        value = value + exchange(value, axis, step)
        step *= 2
    return value


def turn(blocks_ref, factors_ref, *outs):
    pairs = factors_ref.shape[0] // 2
    for index in range(pairs):
        first = 2 * (pairs - 1 - index)
        for ref, block in zip(outs[2 * min(index, 1):], (first, first + 1)):
            ref[max(index - 1, 0)] = jnp.where(block < blocks_ref[0], factors_ref[block], 0.0).T


def shards(columns, vectors, factors, order, blocks, live):
    count, width, rows = vectors.shape[1:]
    slots = columns.shape[2]
    pairs = count // 2
    turns = list(reversed(range(pairs)))

    held = lax.all_to_all(columns[0], "group", split_axis=0, concat_axis=0, tiled=True)

    inside = lax.axis_index("section") * rows + jnp.arange(rows) < order[0]
    basis = jnp.where(inside[None, :], vectors[0].reshape(count * width, rows), jnp.bfloat16(0))
    basis = lax.optimization_barrier(basis)

    def span(low, high):
        return basis[low * width:high * width]

    def product(pair):
        return dot(span(2 * pair + 1, 2 * pair + 2), span(2 * pair, 2 * pair + 1), ROWS)

    last_pair = lax.optimization_barrier(span(count - 2, count))
    gram_first = total(product(turns[0])[None], "section")
    rest = jnp.stack([product(pair) for pair in turns[1:]])
    gram_rest = total(rest, "section")
    outs = [jax.ShapeDtypeStruct((size, width, width), jnp.float32) for size in (1, 1, pairs - 1, pairs - 1)]
    turned = pl.pallas_call(
        turn, out_shape=outs, in_specs=[SMEM, VMEM], out_specs=[VMEM] * 4, name="turn",
    )(blocks, factors[0])

    def merge(gram, lower, higher):
        batch = (((2,), (1,)), ((0,), (0,)))
        corner = -lax.dot_general(
            lax.dot_general(higher, gram, batch, precision=HIGH), lower, batch, precision=HIGH)
        return jnp.concatenate([
            jnp.concatenate([lower, jnp.zeros_like(lower)], axis=2),
            jnp.concatenate([corner, higher], axis=2)], axis=1)

    merged = [merge(gram_first, *turned[:2])[0]]
    rest = merge(gram_rest, *turned[2:])
    merged += [rest[index] for index in range(pairs - 1)]

    peers, half = held.shape[0], held.shape[0] // 2
    me = lax.axis_index("group")
    top = me // half
    panels = []
    for side in (top, 1 - top):
        panels.append(lax.dynamic_slice_in_dim(held, side * half, half, 0).reshape(half * slots, rows))
    for index, pair in enumerate(turns):
        vectors_of = span(2 * pair, 2 * pair + 2)
        for number, panel in enumerate(panels):
            inner = folded(dot(split(panel), vectors_of if index else last_pair, ROWS))
            inner = total(inner, "section")
            weights = dot(inner, merged[index], INNER, HIGH)
            panels[number] = panel - folded(dot(split(weights), vectors_of, INNER))
    result = jnp.zeros_like(held)
    for step in reversed(range(peers)):
        home = me ^ step
        block = lax.dynamic_slice_in_dim(panels[step // half], (home % half) * slots, slots, 0)
        if step:
            block = lax.ppermute(block, "group", [(i, i ^ step) for i in range(peers)])
        result = lax.dynamic_update_slice_in_dim(result, block[None], home, 0)
    keep = jnp.arange(slots)[None, :] < live[0][:, None]
    return jnp.where(keep[:, :, None], result, jnp.float32(0.0))[None]


def solution(mesh):
    return jax.shard_map(
        shards,
        mesh=mesh,
        in_specs=(
            P("group", None, None, "section"),
            P("group", None, None, "section"),
            P("group", None, None, None),
            P("group"),
            P("group"),
            P("group", None),
        ),
        out_specs=P("group", None, None, "section"),
        check_vma=False,
    )
```
